32 devices in a mesh: dp: 4 (over y, core), seq: 8 (over z, x).
Axes of the slice: x: 2, y: 2, z: 4, core: 2. Of those that a mesh axis runs over, the one named last changes fastest.
Arguments:
- tokens: bfloat16 [32768, 2048], P(('dp', 'seq')), parts along dimension 0, may hold values from -6 to 6
- chosen: int32 [4096], P('dp'), parts along dimension 0, may hold values from 0 to 8191, as said below
- gates: float32 [4096], P('dp'), parts along dimension 0, may hold values from 0.5 to 2
- w_query: bfloat16 [2048, 1024], P('seq'), may hold values from -1.8561553 to 1.8561553
- w_key: bfloat16 [2048, 256], P('seq'), may hold values from -0.088388348 to 0.088388348
- w_value: bfloat16 [2048, 256], P('seq'), may hold values from -0.125 to 0.125
- w_out: bfloat16 [1024, 2048], P(None, 'seq'), may hold values from -0.5 to 0.5
Outputs:
- mixed: bfloat16 [32768, 2048], P(('dp', 'seq')), parts along dimension 0
The draws below stay inside these ranges and needn't reach their ends.
There are 4 independent parts, one for each index of `dp`. The reference program is written for one: setup_inputs(seed, part) draws one part's arguments, and reference() takes and returns one part's arrays. A program takes and returns all parts, laid end to end along the dimension named above; an argument that names none is the same for every part. Nothing has to cross between parts.
Inputs may be any that keep to these rules, and one draw needn't show every extreme that they name: `chosen`: distinct positions in increasing order; at most 256 of them lie in one device's 1024 consecutive positions, and exactly 256 lie in some device's positions.
All inputs are finite; a program needn't handle non-finite values.
Results may differ from the reference program's by a relative error of at most 0.006.
Values may be sent and summed in bfloat16 or wider, within the bound.
A program may use at most 128 MiB of HBM per device.

```python
import math
import jax
import jax.numpy as jnp
from jax import lax

D = 2048
HEADS = 8
KV_HEADS = 2
HEAD_DIM = 128
TOK_DEV = 1024
ROWS_DEV = 128
TOKENS = 8192
CHOSEN = 1024
N_SEQ = 8


def draw_chosen(key, part):
    lifts = jax.random.randint(jax.random.fold_in(key, 1), (N_SEQ,), 0, ROWS_DEV + 1)
    heavy = jax.random.randint(jax.random.fold_in(key, 2), (), 0, N_SEQ)
    order = jnp.arange(N_SEQ, dtype=jnp.int32)
    lifts = jnp.where(order == heavy, ROWS_DEV, lifts)
    lifts = jnp.where(order == (heavy + N_SEQ - 1) % N_SEQ, 0, lifts)
    counts = ROWS_DEV + lifts - jnp.roll(lifts, 1)
    subkeys = jax.random.split(jax.random.fold_in(key, 3), N_SEQ)
    ranks = jax.vmap(lambda single: jax.random.permutation(single, TOK_DEV))(subkeys)
    flags = (ranks < counts[:, None]).reshape(-1)
    return jnp.nonzero(flags, size=CHOSEN)[0].astype(jnp.int32)


def shared_base(key):
    raw = jax.random.normal(jax.random.fold_in(key, 11), (D, KV_HEADS * HEAD_DIM), jnp.float32)
    return jnp.clip(raw, -4.0, 4.0) * D ** (-0.5)


def draw_w_key(key, part):
    return shared_base(key).astype(jnp.bfloat16)


def draw_w_query(key, part):
    raw = jax.random.normal(jax.random.fold_in(key, 12), (D, HEADS * HEAD_DIM), jnp.float32)
    noise = jnp.clip(raw, -4.0, 4.0) * 2.0 * D ** (-0.5)
    return noise.astype(jnp.bfloat16)


def steps_of(rng, dims, cuts, least, top_value):
    gain = 1.0
    for position, shards_of in cuts:
        steps = jax.random.uniform(jax.random.fold_in(jax.random.fold_in(rng, 6), position), (shards_of,), jnp.float32, least / len(cuts), top_value / len(cuts))
        gain = gain * jnp.repeat(jnp.exp(steps), dims[position] // shards_of).reshape((-1,) + (1,) * (len(dims) - 1 - position))
    return gain


def bell_draw(rng, dims, spread, limit, cuts=(), kind=jnp.bfloat16):
    drawn = spread * jax.random.normal(rng, dims, jnp.float32)
    if cuts:
        drawn = drawn * steps_of(rng, dims, cuts, -0.22, 0.18)
    return jnp.clip(drawn, -limit, limit).astype(kind)


def setup_inputs(seed: int = 0, part: int = 0) -> dict:
    splits = jax.random.split(jax.random.key(seed), 8)
    part_splits = jax.random.split(jax.random.fold_in(splits[7], part), 8)
    return {
        "tokens": bell_draw(part_splits[0], (TOKENS, D), 1.0, 6.0, ((0, 8),)),
        "chosen": draw_chosen(jax.random.fold_in(jax.random.fold_in(splits[7], part), 71), part),
        "gates": jnp.clip(jax.random.uniform(part_splits[2], (CHOSEN,), jnp.float32, 0.5, 2.0), 0.5, 2.0),
        "w_query": draw_w_query(jax.random.fold_in(splits[7], 71), part),
        "w_key": draw_w_key(jax.random.fold_in(splits[7], 71), part),
        "w_value": bell_draw(splits[5], (D, KV_HEADS * HEAD_DIM), D ** -0.5, 0.125, ((0, 8),)),
        "w_out": bell_draw(splits[6], (HEADS * HEAD_DIM, D), (HEADS * HEAD_DIM // 9) ** -0.5, 0.5, ((1, 8),)),
    }


neg_fill = -1e+30

def reference(tokens, chosen, gates, w_query, w_key, w_value, w_out):
    picked_total = chosen.shape[0]
    group_size = HEADS // KV_HEADS
    block_rows = math.gcd(picked_total, 512)
    picked = tokens[chosen].astype(jnp.float32)
    normed = (picked * lax.rsqrt(lax.optimization_barrier(jnp.mean(picked * picked, axis=1, keepdims=True)) + 1e-06)).astype(jnp.bfloat16)
    query_matrix = (jnp.dot(normed, w_query, preferred_element_type=jnp.float32) * HEAD_DIM ** (-0.5)).astype(jnp.bfloat16)
    keys_all = jnp.dot(normed, w_key, preferred_element_type=jnp.float32).astype(jnp.bfloat16)
    values = jnp.dot(normed, w_value, preferred_element_type=jnp.float32).astype(jnp.bfloat16)
    query_matrix = lax.optimization_barrier(query_matrix).astype(jnp.float32)
    keys_expanded = lax.optimization_barrier(keys_all).astype(jnp.float32).reshape(picked_total, KV_HEADS, HEAD_DIM)
    values_expanded = lax.optimization_barrier(values).astype(jnp.float32).reshape(picked_total, KV_HEADS, HEAD_DIM)
    blocks = query_matrix.reshape(picked_total // block_rows, block_rows, KV_HEADS, group_size, HEAD_DIM)
    firsts = (jnp.arange(picked_total // block_rows, dtype=jnp.int32) * block_rows).astype(jnp.int32)
    key_order = jnp.arange(picked_total, dtype=jnp.int32)

    def one_block(inputs):
        query_tile, first_row = inputs
        logit_scores = jnp.einsum('qjfh,ujh->jfqu', query_tile, keys_expanded)
        query_order = first_row + jnp.arange(block_rows, dtype=jnp.int32)
        allowed = key_order[None, :] <= query_order[:, None]
        logit_scores = jnp.where(allowed, logit_scores, neg_fill)
        top_score = lax.optimization_barrier(jnp.max(logit_scores, axis=-1, keepdims=True))
        probs = jnp.where(allowed, jnp.exp(logit_scores - top_score), 0.0)
        totals = lax.optimization_barrier(jnp.sum(probs, axis=-1))
        softmax_weights = lax.optimization_barrier(probs.astype(jnp.bfloat16)).astype(jnp.float32)
        summed_total = jnp.einsum('yoih,hyf->yoif', softmax_weights, values_expanded)
        attended = summed_total / totals[..., None]
        return jnp.transpose(attended, (2, 0, 1, 3)).reshape(block_rows, HEADS * HEAD_DIM)
    attended = lax.map(one_block, (blocks, firsts)).reshape(picked_total, HEADS * HEAD_DIM).astype(jnp.bfloat16)
    block_out = jnp.dot(attended, w_out, preferred_element_type=jnp.float32).astype(jnp.bfloat16)
    block_wide = lax.optimization_barrier(block_out).astype(jnp.float32)
    mixed = tokens.astype(jnp.float32).at[chosen].add(gates[:, None] * block_wide)
    return mixed.astype(jnp.bfloat16)
```

```python
import functools

import jax
import jax.numpy as jnp
from jax import lax
from jax.experimental import pallas as pl
from jax.experimental.pallas import tpu as pltpu
from jax.sharding import PartitionSpec as P

HEADS = 8
KV_HEADS = 2
HEAD_DIM = 128
MOST_OWN = 256
MESH = pl.DeviceIdType.MESH
NEG = -1e30
F32 = jnp.float32
BF16 = jnp.bfloat16


class Ring:
    def __init__(self, geo, sems, region_in, region_y=None):
        self.g = geo
        self.sems = sems
        self.region_in = region_in
        self.region_y = region_y
        self.sends = []
        a_count, b_count = geo["A"], geo["B"]
        self.order = [(k, 0) for k in range(1, a_count)]
        self.order += [(k, j) for k in range(a_count) for j in range(1, b_count)]

    def piece(self, k, j):
        g = self.g
        a = lax.rem(g["a"] - k + g["A"], g["A"])
        b = lax.rem(g["b"] - j + g["B"], g["B"])
        return a * g["B"] + b

    def copy(self, kind, index, ref, dp, seq):
        send, recv = self.sems[kind]
        return pltpu.make_async_remote_copy(
            src_ref=ref,
            dst_ref=ref,
            send_sem=send.at[index],
            recv_sem=recv.at[index],
            device_id=(dp, seq),
            device_id_type=MESH,
        )

    def send(self, *args):
        made = self.copy(*args)
        made.start()
        self.sends.append(made)

    def arrive(self, kind, index, ref):
        self.copy(kind, index, ref, self.g["dp"], self.g["z_next"]).wait_recv()

    def mine(self, s):
        return self.region_in(s, self.g["y"], self.g["c"])

    def fan(self, k, j):
        if self.region_y is None:
            return
        g = self.g
        index = self.order.index((k, j))
        s = self.piece(k, j)
        self.send("y", index, self.region_y(s, g["y"], g["c"]), g["dp_y"], g["seq"])
        self.send("d", index, self.mine(s), g["dp_c"], g["seq"])

    def slow(self, k):
        g = self.g
        s = self.piece(k, 0)
        if k > 0:
            self.arrive("z", k - 1, self.mine(s))
        if k < g["A"] - 1:
            self.send("z", k, self.mine(s), g["dp"], g["z_next"])
        if g["B"] > 1:
            self.send("x", k * (g["B"] - 1), self.mine(s), g["dp"], g["x_next"])
        if k > 0:
            self.fan(k, 0)

    def fast(self, k, j):
        g = self.g
        s = self.piece(k, j)
        self.arrive("x", k * (g["B"] - 1) + j - 1, self.mine(s))
        if j < g["B"] - 1:
            self.send("x", k * (g["B"] - 1) + j, self.mine(s), g["dp"], g["x_next"])
        self.fan(k, j)

    def relay(self):
        g = self.g
        for index, (k, j) in enumerate(self.order):
            ref = self.region_y(self.piece(k, j), 1 - g["y"], g["c"])
            self.arrive("y", index, ref)
            self.send("d", len(self.order) + index, ref, g["dp_c"], g["seq"])

    def gather_core(self):
        g = self.g
        for index, (k, j) in enumerate(self.order):
            s = self.piece(k, j)
            self.arrive("d", index, self.region_in(s, g["y"], 1 - g["c"]))
            self.arrive("d", len(self.order) + index, self.region_y(s, 1 - g["y"], 1 - g["c"]))

    def finish(self):
        for made in self.sends:
            made.wait_send()


def main_kernel(
    A, B, tok, ch, wq, wk, wv, wo, blk, oh_out,
    tok_v, wbuf, obuf, kvbuf, normed, qs, acc, m_s, l_s, att, lsem,
    wz, wx, wy, wd, oz, ox, oy, od, kz, kx,
):
    n = A * B
    dp = lax.axis_index("dp")
    seq = lax.axis_index("seq")
    a, b = seq // B, lax.rem(seq, B)
    y, c = lax.rem(dp // 2, 2), lax.rem(dp, 2)
    z_next = lax.rem(a + 1, A) * B + b
    z_prev = lax.rem(a + A - 1, A) * B + b
    x_next = a * B + lax.rem(b + 1, B)
    x_prev = a * B + lax.rem(b + B - 1, B)
    dp_y = dp + 2 * (1 - 2 * y)
    dp_c = dp + 1 - 2 * c
    geo = dict(
        A=A, B=B, a=a, b=b, y=y, c=c, dp=dp, seq=seq,
        z_next=z_next, x_next=x_next, dp_y=dp_y, dp_c=dp_c,
    )
    t_rows = tok.shape[0]
    width = tok.shape[1]
    k_rows = wq.shape[0]
    q_cols, e_cols = wq.shape[1], wk.shape[1]
    all_cols = q_cols + 2 * e_cols
    o_rows, o_cols = wo.shape

    rows_here = pl.ds(pl.multiple_of(seq * k_rows, k_rows), k_rows)
    local = [
        (wq, wbuf.at[rows_here, pl.ds(0, q_cols)]),
        (wk, wbuf.at[rows_here, pl.ds(q_cols, e_cols)]),
        (wv, wbuf.at[rows_here, pl.ds(q_cols + e_cols, e_cols)]),
        (wo, obuf.at[seq]),
        (tok, tok_v),
    ]
    local = [pltpu.make_async_copy(s, d, lsem.at[i]) for i, (s, d) in enumerate(local)]
    for made in local:
        made.start()

    greet = [(dp, z_next)] + ([(dp, z_prev)] if A > 2 else [])
    if B > 1:
        greet += [(dp, x_next)] + ([(dp, x_prev)] if B > 2 else [])
    greet += [(dp_y, seq), (dp_c, seq)]
    barrier = pltpu.get_barrier_semaphore()
    for who in greet:
        pl.semaphore_signal(barrier, inc=1, device_id=who, device_id_type=MESH)
    pl.semaphore_wait(barrier, len(greet))

    third = all_cols // 6

    def w_region(s, start, size):
        return wbuf.at[
            pl.ds(pl.multiple_of(s * k_rows, k_rows), k_rows),
            pl.ds(pl.multiple_of(start, 128), size),
        ]

    o_half = o_rows // 2
    o_y = o_half * 3 // 8 // 16 * 16
    o_in = o_half - o_y

    def o_region(s, start, size):
        return obuf.at[s, pl.ds(pl.multiple_of(start, 16), size), :]

    ring_w = Ring(
        geo,
        {"z": wz, "x": wx, "y": wy, "d": wd},
        lambda s, y, c: w_region(s, c * (3 * third) + y * third, 2 * third),
        lambda s, y, c: w_region(s, c * (3 * third) + y * (2 * third), third),
    )
    ring_o = Ring(
        geo,
        {"z": oz, "x": ox, "y": oy, "d": od},
        lambda s, y, c: o_region(s, c * o_half + y * o_y, o_in),
        lambda s, y, c: o_region(s, c * o_half + y * o_in, o_y),
    )
    ring_k = Ring(geo, {"z": kz, "x": kx}, lambda s, y, c: kvbuf.at[s])

    for made in local[:3]:
        made.wait()
    ring_w.slow(0)

    base = seq * t_rows
    picks = ch[...]
    start = jnp.sum((picks < base).astype(F32), axis=1, keepdims=True)
    rel = picks - base
    inside = (rel >= 0) & (rel < t_rows)
    place = jnp.where(inside, (rel + 1).astype(F32), 0.0)
    order = lax.broadcasted_iota(jnp.int32, picks.shape, 1).astype(F32) - start
    slots = lax.broadcasted_iota(jnp.int32, (MOST_OWN, 1), 0).astype(F32)
    own = jnp.sum(jnp.where(order == slots, place, 0.0), axis=1, keepdims=True) - 1.0
    spots = lax.broadcasted_iota(jnp.int32, (1, t_rows), 1).astype(F32)
    oh_out[...] = (own == spots).astype(F32).astype(BF16)
    local[4].wait()
    chunk = 512
    square = jnp.zeros((MOST_OWN, 1), F32)
    for i in range(width // chunk):
        rows = jnp.dot(oh_out[...], tok_v[:, i * chunk : (i + 1) * chunk], preferred_element_type=F32)
        square = square + jnp.sum(rows * rows, axis=1, keepdims=True)
        normed[:, i * chunk : (i + 1) * chunk] = rows.astype(BF16)
    scale = lax.rsqrt(square / width + 1e-06)
    for i in range(width // chunk):
        cols = slice(i * chunk, (i + 1) * chunk)
        normed[:, cols] = (normed[:, cols].astype(F32) * scale).astype(BF16)

    for k in range(1, A):
        ring_w.slow(k)
        for j in range(1, B):
            ring_w.fast(k - 1, j)
    for j in range(1, B):
        ring_w.fast(A - 1, j)
    local[3].wait()
    ring_o.slow(0)
    ring_w.relay()
    ring_w.gather_core()

    kv_cols = 2 * e_cols
    for i in range(kv_cols // 256):
        part = jnp.dot(
            normed[...], wbuf[:, q_cols + i * 256 : q_cols + (i + 1) * 256], preferred_element_type=F32
        )
        kvbuf[seq, :, i * 256 : (i + 1) * 256] = part.astype(BF16)
    ring_k.slow(0)
    group = HEADS // KV_HEADS
    for i in range(q_cols // 256):
        part = jnp.dot(normed[...], wbuf[:, i * 256 : (i + 1) * 256], preferred_element_type=F32)
        part = (part * HEAD_DIM**-0.5).astype(BF16)
        for h in range(2):
            head = i * 2 + h
            first = (head % group) * MOST_OWN
            qs[head // group, first : first + MOST_OWN, :] = part[:, h * 128 : (h + 1) * 128]

    m_s[...] = jnp.full(m_s.shape, NEG, F32)
    l_s[...] = jnp.zeros(l_s.shape, F32)
    acc[...] = jnp.zeros(acc.shape, F32)

    def attend(t, diagonal):
        low = t * t_rows
        count = jnp.sum(
            ((picks >= low) & (picks < low + t_rows)).astype(F32), axis=1, keepdims=True
        )
        col = lax.broadcasted_iota(jnp.int32, (1, MOST_OWN), 1).astype(F32)
        allowed = col < count
        if diagonal:
            row = lax.broadcasted_iota(jnp.int32, (MOST_OWN, MOST_OWN), 0).astype(F32)
            allowed = jnp.logical_and(allowed, col <= row)

        def one(f, _):
            e = f // group
            first = pl.multiple_of(lax.rem(f, group) * MOST_OWN, MOST_OWN)
            rows = pl.ds(first, MOST_OWN)
            ecol = pl.multiple_of(e * HEAD_DIM, HEAD_DIM)
            keys = kvbuf[t, :, pl.ds(ecol, HEAD_DIM)]
            vals = kvbuf[t, :, pl.ds(e_cols + ecol, HEAD_DIM)]
            score = lax.dot_general(
                qs[e, rows, :], keys, (((1,), (1,)), ((), ())), preferred_element_type=F32
            )
            score = jnp.where(allowed, score, NEG)
            old = m_s[e, rows, :]
            top = jnp.maximum(old, jnp.max(score, axis=1, keepdims=True))
            prob = jnp.where(allowed, jnp.exp(score - top[:, :1]), 0.0)
            shrink = jnp.exp(old - top)
            m_s[e, rows, :] = top
            l_s[e, rows, :] = l_s[e, rows, :] * shrink + jnp.sum(prob, axis=1, keepdims=True)
            acc[e, rows, :] = acc[e, rows, :] * shrink + jnp.dot(
                prob.astype(BF16), vals, preferred_element_type=F32
            )
            return 0

        lax.fori_loop(0, HEADS, one, 0)

    def attend_past(t):
        @pl.when(t < seq)
        def _():
            attend(t, False)

    attend(seq, True)
    for k in range(1, A):
        ring_k.slow(k)
        ring_o.slow(k)
        for j in range(1, B):
            ring_k.fast(k - 1, j)
            ring_o.fast(k - 1, j)
        attend_past(ring_k.piece(k, 0))
        for j in range(1, B):
            attend_past(ring_k.piece(k - 1, j))
    for j in range(1, B):
        ring_o.fast(A - 1, j)
    ring_o.relay()
    for j in range(1, B):
        ring_k.fast(A - 1, j)
    for j in range(1, B):
        attend_past(ring_k.piece(A - 1, j))
    for head in range(HEADS):
        first = (head % group) * MOST_OWN
        rows = slice(first, first + MOST_OWN)
        total = l_s[head // group, rows, :]
        total = jnp.where(total > 0.0, total, 1.0)
        att[:, head * HEAD_DIM : (head + 1) * HEAD_DIM] = (
            acc[head // group, rows, :] / total
        ).astype(BF16)
    ring_o.gather_core()
    for s in range(n):
        blk[:, s * o_cols : (s + 1) * o_cols] = jnp.dot(
            att[...], obuf[s], preferred_element_type=F32
        ).astype(BF16)
    ring_w.finish()
    ring_k.finish()
    ring_o.finish()


def add_kernel(tile, tok, ch, gates, oh, blk, out):
    seq = lax.axis_index("seq")
    t_rows = tile * pl.num_programs(0)
    low = seq * t_rows + pl.program_id(0) * tile
    rows = lax.broadcasted_iota(jnp.int32, (tile, 1), 0) + low
    gate = jnp.sum(jnp.where(ch[...] == rows, gates[...], 0.0), axis=1, keepdims=True)
    lift = lax.dot_general(
        oh[...], blk[...], (((0,), (0,)), ((), ())), preferred_element_type=F32
    )
    out[...] = (tok[...].astype(F32) + gate * lift).astype(BF16)


def per_device(tokens, chosen, gates, w_query, w_key, w_value, w_out):
    n = lax.axis_size("seq")
    A = 4 if n % 4 == 0 else 1
    B = n // A
    t_rows, width = tokens.shape
    k_rows, q_cols = w_query.shape
    e_cols = w_key.shape[1]
    all_cols = q_cols + 2 * e_cols
    o_rows, o_cols = w_out.shape
    picks = chosen.reshape(1, -1)
    gate_row = gates.reshape(1, -1)
    dma = pltpu.SemaphoreType.DMA
    any_spec = pl.BlockSpec(memory_space=pl.ANY)
    vmem_spec = pl.BlockSpec(memory_space=pltpu.VMEM)
    steps_x = max(A * (B - 1), 1)

    def pair(count):
        return (dma((count,)), dma((count,)))

    sems = []
    for _ in range(2):
        sems += [pair(A - 1), pair(steps_x), pair(n - 1), pair(2 * (n - 1))]
    sems += [pair(A - 1), pair(steps_x)]
    flat = [x for two in sems for x in two]

    def body(*refs):
        head, tail = refs[: len(refs) - len(flat)], refs[len(refs) - len(flat) :]
        pairs = [(tail[i], tail[i + 1]) for i in range(0, len(tail), 2)]
        main_kernel(A, B, *head, *pairs)

    blk, oh = pl.pallas_call(
        body,
        out_shape=(
            jax.ShapeDtypeStruct((MOST_OWN, width), BF16),
            jax.ShapeDtypeStruct((MOST_OWN, t_rows), BF16),
        ),
        in_specs=[any_spec, vmem_spec] + [any_spec] * 4,
        out_specs=(vmem_spec, vmem_spec),
        scratch_shapes=[
            pltpu.VMEM((t_rows, width), BF16),
            pltpu.VMEM((n * k_rows, all_cols), BF16),
            pltpu.VMEM((n, o_rows, o_cols), BF16),
            pltpu.VMEM((n, MOST_OWN, 2 * e_cols), BF16),
            pltpu.VMEM((MOST_OWN, width), BF16),
            pltpu.VMEM((KV_HEADS, HEADS // KV_HEADS * MOST_OWN, HEAD_DIM), BF16),
            pltpu.VMEM((KV_HEADS, HEADS // KV_HEADS * MOST_OWN, HEAD_DIM), F32),
            pltpu.VMEM((KV_HEADS, HEADS // KV_HEADS * MOST_OWN, HEAD_DIM), F32),
            pltpu.VMEM((KV_HEADS, HEADS // KV_HEADS * MOST_OWN, HEAD_DIM), F32),
            pltpu.VMEM((MOST_OWN, HEADS * HEAD_DIM), BF16),
            dma((5,)),
            *flat,
        ],
        compiler_params=pltpu.CompilerParams(
            collective_id=0, has_side_effects=True, vmem_limit_bytes=60 * 1024 * 1024
        ),
        name="gather_attend",
    )(tokens, picks, w_query, w_key, w_value, w_out)

    tile = 128
    return pl.pallas_call(
        functools.partial(add_kernel, tile),
        grid=(t_rows // tile,),
        out_shape=jax.ShapeDtypeStruct((t_rows, width), BF16),
        in_specs=[
            pl.BlockSpec((tile, width), lambda i: (i, 0)),
            pl.BlockSpec(picks.shape, lambda i: (0, 0)),
            pl.BlockSpec(picks.shape, lambda i: (0, 0)),
            pl.BlockSpec((MOST_OWN, tile), lambda i: (0, i)),
            pl.BlockSpec((MOST_OWN, width), lambda i: (0, 0)),
        ],
        out_specs=pl.BlockSpec((tile, width), lambda i: (i, 0)),
        compiler_params=pltpu.CompilerParams(vmem_limit_bytes=32 * 1024 * 1024),
        name="add_rows",
    )(tokens, picks, gate_row, oh, blk)


def solution(mesh):
    return jax.shard_map(
        per_device,
        mesh=mesh,
        in_specs=(
            P(("dp", "seq"), None),
            P("dp"),
            P("dp"),
            P("seq", None),
            P("seq", None),
            P("seq", None),
            P(None, "seq"),
        ),
        out_specs=P(("dp", "seq"), None),
        check_vma=False,
    )
```

```python
import functools

import jax
import jax.numpy as jnp
from jax import lax
from jax.experimental import pallas as pl
from jax.experimental.pallas import tpu as pltpu
from jax.sharding import PartitionSpec as P

HEADS = 8
KV_HEADS = 2
HEAD_DIM = 128
MOST_OWN = 256
MESH = pl.DeviceIdType.MESH
NEG = -1e30
F32 = jnp.float32
BF16 = jnp.bfloat16


class Ring:
    def __init__(self, geo, sems, region_in, paired=True, causal=False):
        self.g = geo
        self.sems = sems
        self.region_in = region_in
        self.region_y = region_in if paired else None
        self.causal = causal
        self.sends = []
        a_count, b_count = geo["A"], geo["B"]
        self.order = [(k, 0) for k in range(1, a_count)]
        self.order += [(k, j) for k in range(a_count) for j in range(1, b_count)]

    def piece(self, k, j):
        g = self.g
        a = lax.rem(g["a"] - k + g["A"], g["A"])
        b = lax.rem(g["b"] - j + g["B"], g["B"])
        return a * g["B"] + b

    def copy(self, kind, index, ref, dp, seq):
        send, recv = self.sems[kind]
        return pltpu.make_async_remote_copy(
            src_ref=ref,
            dst_ref=ref,
            send_sem=send.at[index],
            recv_sem=recv.at[index],
            device_id=(dp, seq),
            device_id_type=MESH,
        )

    def send(self, *args, when=None):
        made = self.copy(*args)
        self.guard(when, made.start)
        self.sends.append((when, made))

    def guard(self, when, act):
        if when is None:
            act()
        else:
            pl.when(when)(act)

    def fast_needed(self, k, b):
        g = self.g
        if not self.causal:
            return None
        here = g["a"] >= k
        if g["B"] == 2 and k == 0:
            return b == 1
        return here

    def arrive(self, kind, index, ref, when=None):
        self.guard(when, self.copy(kind, index, ref, self.g["dp"], self.g["z_next"]).wait_recv)

    def mine(self, s):
        return self.region_in(s, self.g["y"], self.g["c"])

    def fan(self, k, j):
        if self.region_y is None:
            return
        g = self.g
        index = self.order.index((k, j))
        s = self.piece(k, j)
        self.send("y", index, self.region_y(s, g["y"], g["c"]), g["dp_y"], g["seq"])
        self.send("d", index, self.mine(s), g["dp_c"], g["seq"])

    def slow(self, k):
        g = self.g
        s = self.piece(k, 0)
        came = (g["a"] >= k) if self.causal else None
        goes = jnp.logical_and(g["a"] >= k, g["a"] < g["A"] - 1) if self.causal else None
        if k > 0:
            self.arrive("z", k - 1, self.mine(s), when=came)
        if k < g["A"] - 1:
            self.send("z", k, self.mine(s), g["dp"], g["z_next"], when=goes)
        if g["B"] > 1:
            there = lax.rem(g["b"] + 1, g["B"])
            self.send(
                "x", k * (g["B"] - 1), self.mine(s), g["dp"], g["x_next"], when=self.fast_needed(k, there)
            )
        if k > 0:
            self.fan(k, 0)

    def fast(self, k, j):
        g = self.g
        s = self.piece(k, j)
        need = self.fast_needed(k, g["b"])
        self.arrive("x", k * (g["B"] - 1) + j - 1, self.mine(s), when=need)
        if j < g["B"] - 1:
            self.send("x", k * (g["B"] - 1) + j, self.mine(s), g["dp"], g["x_next"], when=need)
        self.fan(k, j)

    def relay(self):
        g = self.g
        for index, (k, j) in enumerate(self.order):
            ref = self.region_y(self.piece(k, j), 1 - g["y"], g["c"])
            self.arrive("y", index, ref)
            self.send("d", len(self.order) + index, ref, g["dp_c"], g["seq"])

    def gather_core(self):
        g = self.g
        for index, (k, j) in enumerate(self.order):
            s = self.piece(k, j)
            self.arrive("d", index, self.region_in(s, g["y"], 1 - g["c"]))
            self.arrive("d", len(self.order) + index, self.region_y(s, 1 - g["y"], 1 - g["c"]))

    def finish(self):
        for when, made in self.sends:
            self.guard(when, made.wait_send)


def main_kernel(
    A, B, tok, ch, wq, wk, wv, wo, blk, oh_out,
    tok_v, wbuf, obuf, kvbuf, normed, qs, acc, m_s, l_s, att, lsem,
    ez, ex, ey, ed, qz, qx, qy, qd, oz, ox, oy, od, kz, kx,
):
    n = A * B
    dp = lax.axis_index("dp")
    seq = lax.axis_index("seq")
    a, b = seq // B, lax.rem(seq, B)
    y, c = lax.rem(dp // 2, 2), lax.rem(dp, 2)
    z_next = lax.rem(a + 1, A) * B + b
    z_prev = lax.rem(a + A - 1, A) * B + b
    x_next = a * B + lax.rem(b + 1, B)
    x_prev = a * B + lax.rem(b + B - 1, B)
    dp_y = dp + 2 * (1 - 2 * y)
    dp_c = dp + 1 - 2 * c
    geo = dict(
        A=A, B=B, a=a, b=b, y=y, c=c, dp=dp, seq=seq,
        z_next=z_next, x_next=x_next, dp_y=dp_y, dp_c=dp_c,
    )
    t_rows = tok.shape[0]
    width = tok.shape[1]
    k_rows = wq.shape[0]
    q_cols, e_cols = wq.shape[1], wk.shape[1]
    all_cols = q_cols + 2 * e_cols
    o_rows, o_cols = wo.shape

    rows_here = pl.ds(pl.multiple_of(seq * k_rows, k_rows), k_rows)
    local = [
        (wq, wbuf.at[rows_here, pl.ds(0, q_cols)]),
        (wk, wbuf.at[rows_here, pl.ds(q_cols, e_cols)]),
        (wv, wbuf.at[rows_here, pl.ds(q_cols + e_cols, e_cols)]),
        (wo, obuf.at[seq]),
        (tok, tok_v),
    ]
    local = [pltpu.make_async_copy(s, d, lsem.at[i]) for i, (s, d) in enumerate(local)]
    for made in local:
        made.start()

    greet = [(dp, z_next)] + ([(dp, z_prev)] if A > 2 else [])
    if B > 1:
        greet += [(dp, x_next)] + ([(dp, x_prev)] if B > 2 else [])
    greet += [(dp_y, seq), (dp_c, seq)]
    barrier = pltpu.get_barrier_semaphore()
    for who in greet:
        pl.semaphore_signal(barrier, inc=1, device_id=who, device_id_type=MESH)
    pl.semaphore_wait(barrier, len(greet))

    def w_region(s, start, size):
        return wbuf.at[
            pl.ds(pl.multiple_of(s * k_rows, k_rows), k_rows),
            pl.ds(pl.multiple_of(start, 128), size),
        ]

    def quarters(first, size):
        part = size // 4
        return lambda s, y, c: w_region(s, first + (2 * c + y) * part, part)

    o_part = o_rows // 4

    def o_region(s, y, c):
        return obuf.at[s, pl.ds(pl.multiple_of((2 * c + y) * o_part, o_part), o_part), :]

    ring_e = Ring(geo, {"z": ez, "x": ex, "y": ey, "d": ed}, quarters(q_cols, 2 * e_cols))
    ring_q = Ring(geo, {"z": qz, "x": qx, "y": qy, "d": qd}, quarters(0, q_cols))
    ring_o = Ring(geo, {"z": oz, "x": ox, "y": oy, "d": od}, o_region)
    ring_k = Ring(geo, {"z": kz, "x": kx}, lambda s, y, c: kvbuf.at[s], paired=False, causal=True)

    local[1].wait()
    local[2].wait()
    ring_e.slow(0)
    local[0].wait()
    ring_q.slow(0)

    base = seq * t_rows
    picks = ch[...]
    start = jnp.sum((picks < base).astype(F32), axis=1, keepdims=True)
    rel = picks - base
    inside = (rel >= 0) & (rel < t_rows)
    place = jnp.where(inside, (rel + 1).astype(F32), 0.0)
    order = lax.broadcasted_iota(jnp.int32, picks.shape, 1).astype(F32) - start
    slots = lax.broadcasted_iota(jnp.int32, (MOST_OWN, 1), 0).astype(F32)
    own = jnp.sum(jnp.where(order == slots, place, 0.0), axis=1, keepdims=True) - 1.0
    spots = lax.broadcasted_iota(jnp.int32, (1, t_rows), 1).astype(F32)
    oh_out[...] = (own == spots).astype(F32).astype(BF16)
    local[4].wait()
    chunk = 512
    square = jnp.zeros((MOST_OWN, 1), F32)
    for i in range(width // chunk):
        rows = jnp.dot(oh_out[...], tok_v[:, i * chunk : (i + 1) * chunk], preferred_element_type=F32)
        square = square + jnp.sum(rows * rows, axis=1, keepdims=True)
        normed[:, i * chunk : (i + 1) * chunk] = rows.astype(BF16)
    scale = lax.rsqrt(square / width + 1e-06)
    for i in range(width // chunk):
        cols = slice(i * chunk, (i + 1) * chunk)
        normed[:, cols] = (normed[:, cols].astype(F32) * scale).astype(BF16)

    for k in range(1, A):
        for ring in (ring_e, ring_q):
            ring.slow(k)
            for j in range(1, B):
                ring.fast(k - 1, j)
    for j in range(1, B):
        ring_e.fast(A - 1, j)
    local[3].wait()
    ring_o.slow(0)
    ring_e.relay()
    ring_e.gather_core()

    kv_cols = 2 * e_cols
    for i in range(kv_cols // 256):
        part = jnp.dot(
            normed[...], wbuf[:, q_cols + i * 256 : q_cols + (i + 1) * 256], preferred_element_type=F32
        )
        kvbuf[seq, :, i * 256 : (i + 1) * 256] = part.astype(BF16)
    ring_k.slow(0)
    for j in range(1, B):
        ring_q.fast(A - 1, j)
    ring_q.relay()
    ring_q.gather_core()
    group = HEADS // KV_HEADS
    for i in range(q_cols // 256):
        part = jnp.dot(normed[...], wbuf[:, i * 256 : (i + 1) * 256], preferred_element_type=F32)
        part = (part * HEAD_DIM**-0.5).astype(BF16)
        for h in range(2):
            head = i * 2 + h
            first = (head % group) * MOST_OWN
            qs[head // group, first : first + MOST_OWN, :] = part[:, h * 128 : (h + 1) * 128]

    m_s[...] = jnp.full(m_s.shape, NEG, F32)
    l_s[...] = jnp.zeros(l_s.shape, F32)
    acc[...] = jnp.zeros(acc.shape, F32)

    def attend(t, diagonal):
        low = t * t_rows
        count = jnp.sum(
            ((picks >= low) & (picks < low + t_rows)).astype(F32), axis=1, keepdims=True
        )
        col = lax.broadcasted_iota(jnp.int32, (1, MOST_OWN), 1).astype(F32)
        allowed = col < count
        if diagonal:
            row = lax.broadcasted_iota(jnp.int32, (MOST_OWN, MOST_OWN), 0).astype(F32)
            allowed = jnp.logical_and(allowed, col <= row)

        def one(f, _):
            e = f // group
            first = pl.multiple_of(lax.rem(f, group) * MOST_OWN, MOST_OWN)
            rows = pl.ds(first, MOST_OWN)
            ecol = pl.multiple_of(e * HEAD_DIM, HEAD_DIM)
            keys = kvbuf[t, :, pl.ds(ecol, HEAD_DIM)]
            vals = kvbuf[t, :, pl.ds(e_cols + ecol, HEAD_DIM)]
            score = lax.dot_general(
                qs[e, rows, :], keys, (((1,), (1,)), ((), ())), preferred_element_type=F32
            )
            score = jnp.where(allowed, score, NEG)
            old = m_s[e, rows, :]
            top = jnp.maximum(old, jnp.max(score, axis=1, keepdims=True))
            prob = jnp.where(allowed, jnp.exp(score - top[:, :1]), 0.0)
            shrink = jnp.exp(old - top)
            m_s[e, rows, :] = top
            l_s[e, rows, :] = l_s[e, rows, :] * shrink + jnp.sum(prob, axis=1, keepdims=True)
            acc[e, rows, :] = acc[e, rows, :] * shrink + jnp.dot(
                prob.astype(BF16), vals, preferred_element_type=F32
            )
            return 0

        lax.fori_loop(0, HEADS, one, 0)

    def attend_past(t):
        @pl.when(t < seq)
        def _():
            attend(t, False)

    attend(seq, True)
    for k in range(1, A):
        ring_k.slow(k)
        ring_o.slow(k)
        for j in range(1, B):
            ring_k.fast(k - 1, j)
            ring_o.fast(k - 1, j)
        attend_past(ring_k.piece(k, 0))
        for j in range(1, B):
            attend_past(ring_k.piece(k - 1, j))
    for j in range(1, B):
        ring_o.fast(A - 1, j)
    ring_o.relay()
    for j in range(1, B):
        ring_k.fast(A - 1, j)
    for j in range(1, B):
        attend_past(ring_k.piece(A - 1, j))
    for head in range(HEADS):
        first = (head % group) * MOST_OWN
        rows = slice(first, first + MOST_OWN)
        total = l_s[head // group, rows, :]
        total = jnp.where(total > 0.0, total, 1.0)
        att[:, head * HEAD_DIM : (head + 1) * HEAD_DIM] = (
            acc[head // group, rows, :] / total
        ).astype(BF16)
    ring_o.gather_core()
    for s in range(n):
        blk[:, s * o_cols : (s + 1) * o_cols] = jnp.dot(
            att[...], obuf[s], preferred_element_type=F32
        ).astype(BF16)
    ring_e.finish()
    ring_q.finish()
    ring_k.finish()
    ring_o.finish()


def add_kernel(tile, tok, ch, gates, oh, blk, out):
    seq = lax.axis_index("seq")
    t_rows = tile * pl.num_programs(0)
    low = seq * t_rows + pl.program_id(0) * tile
    rows = lax.broadcasted_iota(jnp.int32, (tile, 1), 0) + low
    gate = jnp.sum(jnp.where(ch[...] == rows, gates[...], 0.0), axis=1, keepdims=True)
    lift = lax.dot_general(
        oh[...], blk[...], (((0,), (0,)), ((), ())), preferred_element_type=F32
    )
    out[...] = (tok[...].astype(F32) + gate * lift).astype(BF16)


def per_device(tokens, chosen, gates, w_query, w_key, w_value, w_out):
    n = lax.axis_size("seq")
    A = 4 if n % 4 == 0 else 1
    B = n // A
    t_rows, width = tokens.shape
    k_rows, q_cols = w_query.shape
    e_cols = w_key.shape[1]
    all_cols = q_cols + 2 * e_cols
    o_rows, o_cols = w_out.shape
    picks = chosen.reshape(1, -1)
    gate_row = gates.reshape(1, -1)
    dma = pltpu.SemaphoreType.DMA
    any_spec = pl.BlockSpec(memory_space=pl.ANY)
    vmem_spec = pl.BlockSpec(memory_space=pltpu.VMEM)
    steps_x = max(A * (B - 1), 1)

    def pair(count):
        return (dma((count,)), dma((count,)))

    sems = []
    for _ in range(3):
        sems += [pair(A - 1), pair(steps_x), pair(n - 1), pair(2 * (n - 1))]
    sems += [pair(A - 1), pair(steps_x)]
    flat = [x for two in sems for x in two]

    def body(*refs):
        head, tail = refs[: len(refs) - len(flat)], refs[len(refs) - len(flat) :]
        pairs = [(tail[i], tail[i + 1]) for i in range(0, len(tail), 2)]
        main_kernel(A, B, *head, *pairs)

    blk, oh = pl.pallas_call(
        body,
        out_shape=(
            jax.ShapeDtypeStruct((MOST_OWN, width), BF16),
            jax.ShapeDtypeStruct((MOST_OWN, t_rows), BF16),
        ),
        in_specs=[any_spec, vmem_spec] + [any_spec] * 4,
        out_specs=(vmem_spec, vmem_spec),
        scratch_shapes=[
            pltpu.VMEM((t_rows, width), BF16),
            pltpu.VMEM((n * k_rows, all_cols), BF16),
            pltpu.VMEM((n, o_rows, o_cols), BF16),
            pltpu.VMEM((n, MOST_OWN, 2 * e_cols), BF16),
            pltpu.VMEM((MOST_OWN, width), BF16),
            pltpu.VMEM((KV_HEADS, HEADS // KV_HEADS * MOST_OWN, HEAD_DIM), BF16),
            pltpu.VMEM((KV_HEADS, HEADS // KV_HEADS * MOST_OWN, HEAD_DIM), F32),
            pltpu.VMEM((KV_HEADS, HEADS // KV_HEADS * MOST_OWN, HEAD_DIM), F32),
            pltpu.VMEM((KV_HEADS, HEADS // KV_HEADS * MOST_OWN, HEAD_DIM), F32),
            pltpu.VMEM((MOST_OWN, HEADS * HEAD_DIM), BF16),
            dma((5,)),
            *flat,
        ],
        compiler_params=pltpu.CompilerParams(
            collective_id=0, has_side_effects=True, vmem_limit_bytes=60 * 1024 * 1024
        ),
        name="gather_attend",
    )(tokens, picks, w_query, w_key, w_value, w_out)

    tile = 128
    return pl.pallas_call(
        functools.partial(add_kernel, tile),
        grid=(t_rows // tile,),
        out_shape=jax.ShapeDtypeStruct((t_rows, width), BF16),
        in_specs=[
            pl.BlockSpec((tile, width), lambda i: (i, 0)),
            pl.BlockSpec(picks.shape, lambda i: (0, 0)),
            pl.BlockSpec(picks.shape, lambda i: (0, 0)),
            pl.BlockSpec((MOST_OWN, tile), lambda i: (0, i)),
            pl.BlockSpec((MOST_OWN, width), lambda i: (0, 0)),
        ],
        out_specs=pl.BlockSpec((tile, width), lambda i: (i, 0)),
        compiler_params=pltpu.CompilerParams(vmem_limit_bytes=62 * 1024 * 1024),
        name="add_rows",
    )(tokens, picks, gate_row, oh, blk)


def solution(mesh):
    return jax.shard_map(
        per_device,
        mesh=mesh,
        in_specs=(
            P(("dp", "seq"), None),
            P("dp"),
            P("dp"),
            P("seq", None),
            P("seq", None),
            P("seq", None),
            P(None, "seq"),
        ),
        out_specs=P(("dp", "seq"), None),
        check_vma=False,
    )
```
